256 devices in a mesh: dp: 256 (over z, x, y, core).
Axes of the slice: x: 4, y: 4, z: 8, core: 2. Of those that a mesh axis runs over, the one named last changes fastest.
Arguments:
- images: bfloat16 [1024, 92, 4096], P('dp'), may hold values from -6 to 6
- layer_gain: float32 [4096], replicated, may hold values from 0.5 to 1.5
- in_weight: bfloat16 [4096, 1024], replicated, may hold values from -1 to 1
- out_weight: bfloat16 [1024, 1024], replicated, may hold values from -1 to 1
- text_embed: bfloat16 [1024, 1024], P('dp'), may hold values from -6 to 6
- pair_index: int32 [1024], P('dp'), may hold values from 0 to 1023, each once
- logit_scale: float32 [1], replicated, may hold values from 30 to 200
Outputs:
- loss: float32 [1], replicated
- grad_norm: float32 [1], replicated
- update_image: float32 [1024, 1024], P('dp')
- update_text: float32 [1024, 1024], P('dp')
The draws below stay inside these ranges and needn't reach their ends.
Inputs may be any that keep to these rules, and one draw needn't show every extreme that they name: Image i is paired with text row pair_index[i]; every text row is paired with exactly one image.
All inputs are finite; a program needn't handle non-finite values.
Results may differ from the reference program's by a relative error of at most 0.0086.
Values may be sent and summed in bfloat16 or wider, within the bound.
A program may use at most 64 MiB of HBM per device.

```python
import math
from functools import partial
import jax
import jax.numpy as jnp
from jax import lax

E = 1024
PS = 4096
TT = 92
B_DEV = 4
BATCH = 1024


encoded_count = 64


rise_weight = 1.5


EPS_LAYER = 1e-05


def gain_values(key):
    noise = jax.random.normal(jax.random.fold_in(key, 301), (PS,), jnp.float32)
    return jnp.clip(1.0 + 0.1 * noise, 0.5, 1.5)


def input_matrix(key):
    noise = jax.random.normal(jax.random.fold_in(key, 303), (PS, E), jnp.float32)
    return jnp.clip(noise / math.sqrt(PS), -1.0, 1.0)


def output_matrix(key):
    noise = jax.random.normal(jax.random.fold_in(key, 305), (E, E), jnp.float32)
    return jnp.clip(noise / math.sqrt(E), -1.0, 1.0)


def draw_layer_gain(key, part):
    return gain_values(key)


def draw_in_weight(key, part):
    return input_matrix(key).astype(jnp.bfloat16)


def draw_out_weight(key, part):
    return output_matrix(key).astype(jnp.bfloat16)


def base_vector(key, row):
    return jax.random.normal(jax.random.fold_in(jax.random.fold_in(key, 101), row), (PS,), jnp.float32)


def token_noise(key, row):
    return jax.random.normal(jax.random.fold_in(jax.random.fold_in(key, 103), row), (TT, PS), jnp.float32)


def copied_row(key, row):
    device = row // B_DEV
    leader = jnp.where(device % 2 == 1, device * B_DEV, row)
    lead_base = base_vector(key, leader)
    lead_tokens = token_noise(key, leader)
    own_tokens = token_noise(key, row)
    extra = jnp.where(leader == row, 0.0, 0.01)
    mixed = 0.8 * lead_base[None, :] + 0.6 * lead_tokens + extra * own_tokens
    return jnp.clip(mixed, -6.0, 6.0).astype(jnp.bfloat16)


def draw_images(key, part):
    rows = jnp.arange(BATCH, dtype=jnp.int32)
    result = lax.map(lambda row: copied_row(key, row), rows)
    return result


def encode_images_drawn(pixels, layer_gain, in_weight, out_weight):
    values = pixels.astype(jnp.float32)
    average = jnp.mean(values, axis=-1, keepdims=True)
    centered = values - average
    variance = jnp.mean(centered * centered, axis=-1, keepdims=True)
    normed = (centered * lax.rsqrt(variance + EPS_LAYER) * layer_gain).astype(jnp.bfloat16)
    flattened = normed.reshape(-1, normed.shape[-1])
    hidden = jax.nn.gelu(jnp.dot(flattened, in_weight, preferred_element_type=jnp.float32), approximate=True)
    pooled = jnp.mean(hidden.reshape(pixels.shape[0], pixels.shape[1], -1), axis=1).astype(jnp.bfloat16)
    return jnp.dot(pooled, out_weight, preferred_element_type=jnp.float32)


def normalized(vector):
    return vector / jnp.sqrt(jnp.sum(vector * vector, axis=-1, keepdims=True))


def common_direction(key):
    rows = jnp.arange(encoded_count, dtype=jnp.int32)
    pixels = lax.map(lambda row: copied_row(key, row), rows)
    embedded = encode_images_drawn(pixels, gain_values(key), input_matrix(key).astype(jnp.bfloat16), output_matrix(key).astype(jnp.bfloat16))
    return normalized(jnp.mean(normalized(embedded), axis=0))


def rising_texts(key):
    noise = jax.random.normal(jax.random.fold_in(key, 231), (BATCH, E), jnp.float32)
    direction = common_direction(key)
    ranks = jnp.arange(BATCH, dtype=jnp.float32) / BATCH
    texts = noise - rise_weight * math.sqrt(E) * ranks[:, None] * direction[None, :]
    return jnp.clip(texts, -6.0, 6.0)


def draw_text_embed(key, part):
    texts = rising_texts(key)
    return texts.astype(jnp.bfloat16)


def draw_logit_scale(key, part):
    scale_key = jax.random.fold_in(key, 601)
    value = jnp.exp(jax.random.uniform(scale_key, (1,), jnp.float32, math.log(30.0), math.log(200.0)))
    return value


def setup_inputs(seed: int = 0) -> dict:
    key_list = jax.random.split(jax.random.key(seed), 8)
    images = draw_images(jax.random.fold_in(key_list[7], 71), 0)
    layer_gain = draw_layer_gain(jax.random.fold_in(key_list[7], 71), 0)
    in_weight = draw_in_weight(jax.random.fold_in(key_list[7], 71), 0)
    out_weight = draw_out_weight(jax.random.fold_in(key_list[7], 71), 0)
    text_embed = draw_text_embed(jax.random.fold_in(key_list[7], 71), 0)
    pair_index = jax.random.permutation(key_list[5], BATCH).astype(jnp.int32)
    logit_scale = draw_logit_scale(jax.random.fold_in(key_list[7], 71), 0)
    return dict(images=images, layer_gain=layer_gain, in_weight=in_weight, out_weight=out_weight, text_embed=text_embed, pair_index=pair_index, logit_scale=logit_scale)


EPS_UNIT = 1e-06
EPS_LAYER = 1e-05

def encode_images(pixels, layer_gain, in_weight, out_weight):
    values = pixels.astype(jnp.float32)
    average = lax.optimization_barrier(jnp.mean(values, axis=-1, keepdims=True))
    centered = values - average
    variance = lax.optimization_barrier(jnp.mean(centered * centered, axis=-1, keepdims=True))
    normed = (centered * lax.rsqrt(variance + EPS_LAYER) * layer_gain).astype(jnp.bfloat16)
    flattened = normed.reshape(-1, normed.shape[-1])
    hidden = jax.nn.gelu(jnp.dot(flattened, in_weight, preferred_element_type=jnp.float32), approximate=True)
    pooled = lax.optimization_barrier(jnp.mean(hidden.reshape(pixels.shape[0], pixels.shape[1], -1), axis=1)).astype(jnp.bfloat16)
    return jnp.dot(pooled, out_weight, preferred_element_type=jnp.float32)

def unit_rows(matrix):
    length = jnp.sqrt(lax.optimization_barrier(jnp.sum(matrix * matrix, axis=1, keepdims=True)) + EPS_UNIT)
    return (matrix / length, length)

def unit_backward(grad_unit, unit_vec, length):
    return (grad_unit - unit_vec * lax.optimization_barrier(jnp.sum(unit_vec * grad_unit, axis=1, keepdims=True))) / length

def reference(images, layer_gain, in_weight, out_weight, text_embed, pair_index, logit_scale):
    multiplier = logit_scale[0]
    blocks = images.reshape(BATCH // B_DEV, B_DEV, TT, PS)
    encoder = partial(encode_images, layer_gain=layer_gain, in_weight=in_weight, out_weight=out_weight)
    image_emb = lax.map(encoder, blocks).reshape(BATCH, -1)
    image_unit, image_len = unit_rows(image_emb)
    image_vec = image_unit.astype(jnp.bfloat16)
    text_unit, text_len = unit_rows(text_embed.astype(jnp.float32))
    text_vec = text_unit.astype(jnp.bfloat16)
    scores = multiplier * jnp.dot(image_vec, text_vec.T, preferred_element_type=jnp.float32)
    row_high = lax.optimization_barrier(jnp.max(scores, axis=1, keepdims=True))
    row_lse = row_high[:, 0] + jnp.log(lax.optimization_barrier(jnp.sum(jnp.exp(scores - row_high), axis=1)))
    col_high = lax.optimization_barrier(jnp.max(scores, axis=0, keepdims=True))
    col_lse = col_high[0, :] + jnp.log(lax.optimization_barrier(jnp.sum(jnp.exp(scores - col_high), axis=0)))
    target = jnp.arange(BATCH, dtype=jnp.int32)[None, :] == pair_index[:, None]
    positive = lax.optimization_barrier(jnp.sum(jnp.where(target, scores, jnp.zeros_like(scores)), axis=1))
    loss = (jnp.sum(row_lse) + jnp.sum(col_lse) - 2.0 * jnp.sum(positive)) / (2.0 * BATCH)
    weights = (jnp.exp(scores - row_lse[:, None]) + jnp.exp(scores - col_lse[None, :]) - 2.0 * target.astype(jnp.float32)).astype(jnp.bfloat16)
    grad_image_unit = multiplier * jnp.dot(weights, text_vec, preferred_element_type=jnp.float32)
    grad_text_unit = multiplier * jnp.dot(weights.T, image_vec, preferred_element_type=jnp.float32)
    grad_image = unit_backward(grad_image_unit, image_unit, image_len)
    grad_text = unit_backward(grad_text_unit, text_unit, text_len)
    squares = jnp.sum(grad_image * grad_image) + jnp.sum(grad_text * grad_text)
    factor = lax.rsqrt(squares / (2.0 * BATCH * E) + 1e-06)
    return (loss.reshape(1), jnp.sqrt(squares).reshape(1), grad_image * factor, grad_text * factor)
```

```python
import functools

import jax
import jax.numpy as jnp
from jax import lax
from jax.experimental import pallas as pl
from jax.experimental.pallas import tpu as pltpu
from jax.sharding import Mesh
from jax.sharding import PartitionSpec as P

AXES = ("z", "x", "y", "c")
NZ, NX, NY = 8, 4, 4
EPS_UNIT = 1e-06
EPS_LAYER = 1e-05
F32 = jnp.float32
BF16 = jnp.bfloat16
TOKENS, WIDE, E, HALF, ROWS = 92, 4096, 1024, 512, 1024
PAD = 96


def coordinates():
    return tuple(lax.axis_index(a) for a in AXES)


def remote(src, dst, send_sem, recv_sem, where):
    return pltpu.make_async_remote_copy(
        src_ref=src,
        dst_ref=dst,
        send_sem=send_sem,
        recv_sem=recv_sem,
        device_id=where,
        device_id_type=pl.DeviceIdType.MESH,
    )


Z_ORDER = (4, 3, 5, 2, 6, 1, 7, 0)
RING = (2, 1, 3)


class Gather:
    def __init__(self, place, send, line, whole, sems):
        self.z, self.x, self.y, self.c = place
        self.send, self.line, self.whole = send, line, whole
        (self.s1, self.r1, self.s2, self.r2, self.s3, self.r3, self.s4, self.r4) = sems
        self.copies = []
        self.second = {}
        self.third = {}
        self.cross = {}

    def block(self, q, p):
        c = self.c
        x = lax.rem(self.x + NX - q * (1 - c) + NX - p * c, NX)
        y = lax.rem(self.y + NY - q * c + NY - p * (1 - c), NY)
        return x * NY + y

    def start_line(self):
        j = self.c * NZ + self.z
        self.first = []
        for oz in Z_ORDER:
            for oc in range(2):
                if oz == 0 and oc == 0:
                    continue
                tz, tc = lax.rem(self.z + oz, NZ), lax.rem(self.c + oc, 2)
                o = oz * 2 + oc
                copy = remote(
                    self.send.at[tc], self.line.at[j], self.s1.at[o], self.r1.at[o], (tz, self.x, self.y, tc)
                )
                copy.start()
                self.first.append(copy)
        self.line[j] = self.send[self.c]
        self.copies += self.first

    def finish_line(self):
        for copy in self.first:
            copy.wait_recv()
        c, b = self.c, self.block(0, 0)
        for j in range(2 * NZ):
            r = (j % NZ) * 4
            self.whole[c, j // NZ, b, r : r + 4, :] = self.line[j]

    def start_second(self):
        c, b = self.c, self.block(0, 0)
        here = self.whole.at[c, :, b]
        for o in RING:
            where = (self.z, lax.rem(self.x + o * (1 - c), NX), lax.rem(self.y + o * c, NY), c)
            copy = remote(here, here, self.s2.at[o], self.r2.at[o], where)
            copy.start()
            self.second[o] = copy
            self.copies.append(copy)
        self.forward(0)

    def to_partner(self, q, p):
        here = self.whole.at[self.c, :, self.block(q, p)]
        copy = remote(here, here, self.s4.at[q * 4 + p], self.r4.at[q * 4 + p], (self.z, self.x, self.y, 1 - self.c))
        copy.start()
        self.cross[q, p] = copy
        self.copies.append(copy)

    def forward(self, q):
        c = self.c
        here = self.whole.at[c, :, self.block(q, 0)]
        for p in RING:
            where = (self.z, lax.rem(self.x + p * c, NX), lax.rem(self.y + p * (1 - c), NY), c)
            copy = remote(here, here, self.s3.at[q * 4 + p], self.r3.at[q * 4 + p], where)
            copy.start()
            self.third[q, p] = copy
            self.copies.append(copy)
        self.to_partner(q, 0)

    def finish_second(self):
        for o in (1, 3, 2):
            self.second[o].wait_recv()
            self.forward(o)

    def finish_third(self):
        for q in (0, 1, 3, 2):
            for p in (1, 3, 2):
                self.third[q, p].wait_recv()
                self.to_partner(q, p)

    def finish_cross(self):
        for q in (0, 1, 3, 2):
            for p in (0, 1, 3, 2):
                self.cross[q, p].wait_recv()

    def drain(self):
        for copy in self.copies:
            copy.wait_send()


class SmallGather:
    def __init__(self, place, send, line, whole, sems):
        self.z, self.x, self.y, self.c = place
        self.send, self.line, self.whole = send, line, whole
        (self.s1, self.r1, self.s2, self.r2, self.s3, self.r3) = sems
        self.copies = []
        self.second = {}
        self.third = {}

    block = Gather.block

    def start_line(self):
        j = self.c * NZ + self.z
        self.first = []
        for oz in Z_ORDER:
            for oc in range(2):
                if oz == 0 and oc == 0:
                    continue
                tz, tc = lax.rem(self.z + oz, NZ), lax.rem(self.c + oc, 2)
                o = oz * 2 + oc
                copy = remote(self.send, self.line.at[j], self.s1.at[o], self.r1.at[o], (tz, self.x, self.y, tc))
                copy.start()
                self.first.append(copy)
        self.line[j] = self.send[...]
        self.copies += self.first

    def finish_line(self):
        for copy in self.first:
            copy.wait_recv()
        total = self.line[0]
        for j in range(1, 2 * NZ):
            total = total + self.line[j]
        self.whole[self.block(0, 0)] = total

    def start_second(self):
        c = self.c
        here = self.whole.at[self.block(0, 0)]
        for o in RING:
            where = (self.z, lax.rem(self.x + o * (1 - c), NX), lax.rem(self.y + o * c, NY), c)
            copy = remote(here, here, self.s2.at[o], self.r2.at[o], where)
            copy.start()
            self.second[o] = copy
            self.copies.append(copy)
        self.forward(0)

    def forward(self, q):
        c = self.c
        here = self.whole.at[self.block(q, 0)]
        for p in RING:
            where = (self.z, lax.rem(self.x + p * c, NX), lax.rem(self.y + p * (1 - c), NY), c)
            copy = remote(here, here, self.s3.at[q * 4 + p], self.r3.at[q * 4 + p], where)
            copy.start()
            self.third[q, p] = copy
            self.copies.append(copy)

    def finish_second(self):
        for o in (1, 3, 2):
            self.second[o].wait_recv()
            self.forward(o)

    def finish_third(self):
        for q in (0, 1, 3, 2):
            for p in (1, 3, 2):
                self.third[q, p].wait_recv()

    drain = Gather.drain


def spread(values, first_lane):
    lanes = lax.broadcasted_iota(jnp.int32, (4, 128), 1) - lax.broadcasted_iota(jnp.int32, (4, 128), 0)
    return jnp.sum(jnp.where(lanes == first_lane, values, 0.0), axis=0, keepdims=True)


def unit_rows(matrix):
    length = jnp.sqrt(jnp.sum(matrix * matrix, axis=1, keepdims=True) + EPS_UNIT)
    return matrix / length, length


def columns_of(whole, out, kinds):
    eye = lax.broadcasted_iota(jnp.int32, (128, 128), 0) == lax.broadcasted_iota(jnp.int32, (128, 128), 1)
    for b in range(NX * NY):
        column = jnp.sum(jnp.where(eye, jnp.broadcast_to(whole[b], (128, 128)), 0.0), axis=1, keepdims=True)
        for k in range(kinds):
            out[k, b * 32 : b * 32 + 32, :] = column[k * 32 : k * 32 + 32]


def kernel(
    images, gain, in_weight, out_weight, text, pair, scale,
    loss, norm, update_image, update_text,
    pixels, normed, w, ow, pooled,
    text_send, text_line, text_all, image_send, image_line, image_all,
    tag_send, tag_line, tag_all, len_send, len_line, len_all,
    scores, weights, row_lse, tags, lens, grad, own, swap_out, swap_in,
    load_sem, swap_sem, *sems,
):
    place = coordinates()
    z, x, y, c = place
    text_gather = Gather(place, text_send, text_line, text_all, sems[0:8])
    image_gather = Gather(place, image_send, image_line, image_all, sems[8:16])
    tag_gather = SmallGather(place, tag_send, tag_line, tag_all, sems[16:22])
    len_gather = SmallGather(place, len_send, len_line, len_all, sems[22:28])

    loads = []
    for i in range(4):
        loads.append(pltpu.make_async_copy(images.at[i], pixels.at[i], load_sem.at[i]))
    for n in range(4):
        part = pl.ds(n * 256, 256)
        loads.append(pltpu.make_async_copy(in_weight.at[:, part], w.at[n], load_sem.at[4 + n]))
    loads.append(pltpu.make_async_copy(out_weight, ow, load_sem.at[8]))
    for copy in loads:
        copy.start()

    barrier = pltpu.get_barrier_semaphore()
    peers = []
    for oz in range(NZ):
        for oc in range(2):
            if oz or oc:
                peers.append((lax.rem(z + oz, NZ), x, y, lax.rem(c + oc, 2)))
    for o in (1, 2, 3):
        peers.append((z, lax.rem(x + o, NX), y, c))
        peers.append((z, x, lax.rem(y + o, NY), c))
    for where in peers:
        pl.semaphore_signal(barrier, inc=1, device_id=where, device_id_type=pl.DeviceIdType.MESH)

    text_unit, text_len = unit_rows(text[...].astype(F32))
    text_vec = text_unit.astype(BF16)
    for k in range(2):
        text_send[k] = text_vec[:, k * HALF : (k + 1) * HALF]
    lane = lax.broadcasted_iota(jnp.int32, (1, 128), 1)
    first_lane = (c * NZ + z) * 4
    tag = spread(text_len, first_lane + 64)
    for i in range(4):
        t = pair[i]
        row = (((t >> 2) & 1) << 9) | (((t >> 5) & 3) << 7) | (((t >> 3) & 3) << 5) | ((t >> 7) << 2) | (t & 3)
        tag = tag + jnp.where(lane == first_lane + i, row.astype(F32), 0.0)
    tag_send[...] = tag

    pl.semaphore_wait(barrier, len(peers))
    text_gather.start_line()
    tag_gather.start_line()

    def normalise(i, carry):
        for start in range(0, TOKENS, 32):
            size = min(32, TOKENS - start)
            rows = pl.ds(start, size)
            total = jnp.zeros((size, 128), F32)
            for k in range(WIDE // 128):
                total = total + pixels[i, rows, k * 128 : (k + 1) * 128].astype(F32)
            average = jnp.sum(total, axis=1, keepdims=True) * (1.0 / WIDE)
            total = jnp.zeros((size, 128), F32)
            for k in range(WIDE // 128):
                centered = pixels[i, rows, k * 128 : (k + 1) * 128].astype(F32) - average
                total = total + centered * centered
            variance = jnp.sum(total, axis=1, keepdims=True) * (1.0 / WIDE)
            factor = lax.rsqrt(variance + EPS_LAYER)
            for k in range(WIDE // 128):
                part = slice(k * 128, (k + 1) * 128)
                centered = pixels[i, rows, part].astype(F32) - average
                normed[i, rows, part] = (centered * factor * gain[:, part]).astype(BF16)
        return carry

    for i in range(4):
        loads[i].wait()
    normed[:, 80:PAD, :] = jnp.zeros((4, 16, WIDE), BF16)
    lax.fori_loop(0, 4, normalise, 0)

    text_gather.finish_line()
    tag_gather.finish_line()
    text_gather.start_second()
    tag_gather.start_second()

    pooled[...] = jnp.zeros_like(pooled)
    for n in range(4):
        loads[4 + n].wait()

    def encode(n, carry):
        flat = normed[...].reshape(4 * PAD, WIDE)
        hidden = jax.nn.gelu(jnp.dot(flat, w[n], preferred_element_type=F32), approximate=True)
        for i in range(4):
            mean = jnp.sum(hidden[i * PAD : i * PAD + TOKENS], axis=0, keepdims=True) * (1.0 / TOKENS)
            pooled[n, i : i + 1, :] = mean
        return carry

    lax.fori_loop(0, 2, encode, 0)
    text_gather.finish_second()
    tag_gather.finish_second()
    lax.fori_loop(2, 4, encode, 0)
    loads[8].wait()
    image_emb = jnp.zeros((8, E), F32)
    for n in range(4):
        image_emb = image_emb + jnp.dot(
            pooled[n].astype(BF16), ow[n * 256 : (n + 1) * 256, :], preferred_element_type=F32
        )
    image_unit, image_len = unit_rows(image_emb[0:4])
    image_vec = image_unit.astype(BF16)
    for k in range(2):
        image_send[k] = image_vec[:, k * HALF : (k + 1) * HALF]
    len_send[...] = spread(image_len, first_lane)
    image_gather.start_line()
    len_gather.start_line()

    text_gather.finish_third()
    tag_gather.finish_third()
    columns_of(tag_all, tags, 4)
    image_gather.finish_line()
    len_gather.finish_line()
    image_gather.start_second()
    len_gather.start_second()
    text_gather.finish_cross()
    image_gather.finish_second()
    len_gather.finish_second()
    image_gather.finish_third()
    len_gather.finish_third()
    image_gather.finish_cross()
    columns_of(len_all, lens, 2)

    multiplier = scale[0]

    def score(chunk, carry):
        side, b = chunk // 2, (chunk % 2) * 8
        total = jnp.zeros((256, ROWS), F32)
        for k in range(2):
            total = total + lax.dot_general(
                image_all[k, side, pl.ds(b, 8)].reshape(256, HALF),
                text_all[k].reshape(ROWS, HALF),
                (((1,), (1,)), ((), ())),
                preferred_element_type=F32,
            )
        scores[pl.ds(pl.multiple_of(chunk * 256, 256), 256), :] = total * multiplier
        return carry

    lax.fori_loop(0, 4, score, 0)

    def over_rows(r, high):
        rows = pl.ds(pl.multiple_of(r * 32, 32), 32)
        s = scores[rows, :]
        top = jnp.max(s, axis=1, keepdims=True)
        row_lse[rows, :] = top + jnp.log(jnp.sum(jnp.exp(s - top), axis=1, keepdims=True))
        return jnp.maximum(high, jnp.max(s.reshape(4, 8, ROWS), axis=0))

    high = lax.fori_loop(0, 32, over_rows, jnp.full((8, ROWS), -jnp.inf, F32))
    high = jnp.max(high, axis=0, keepdims=True)

    def over_columns(r, total):
        rows = pl.ds(pl.multiple_of(r * 32, 32), 32)
        return total + jnp.sum(jnp.exp(scores[rows, :] - high).reshape(4, 8, ROWS), axis=0)

    total = lax.fori_loop(0, 32, over_columns, jnp.zeros((8, ROWS), F32))
    col_lse = high + jnp.log(jnp.sum(total, axis=0, keepdims=True))

    ids = lax.broadcasted_iota(jnp.int32, (32, ROWS), 1).astype(F32)

    def weigh(r, positive):
        rows = pl.ds(pl.multiple_of(r * 32, 32), 32)
        s = scores[rows, :]
        hit = ids == tags[r // 16, pl.ds(pl.multiple_of((r % 16) * 32, 32), 32), :]
        value = jnp.exp(s - row_lse[rows, :]) + jnp.exp(s - col_lse) - jnp.where(hit, 2.0, 0.0)
        weights[r // 16, pl.ds(pl.multiple_of((r % 16) * 32, 32), 32), :] = value.astype(BF16)
        return positive + jnp.sum(jnp.where(hit, s, 0.0).reshape(4, 8, ROWS), axis=0)

    positive = lax.fori_loop(0, 32, weigh, jnp.zeros((8, ROWS), F32))
    loss[0] = (jnp.sum(row_lse[...]) + jnp.sum(col_lse) - 2.0 * jnp.sum(positive)) * (0.5 / ROWS)

    squares = jnp.zeros((HALF, 1), F32)
    b = x * NY + y
    for side in range(2):
        vectors = image_all if side == 0 else text_all
        others = text_all if side == 0 else image_all
        size = jnp.zeros((HALF, 1), F32)
        along = jnp.zeros((HALF, 1), F32)
        for k in range(2):
            if side == 0:
                left = weights[c]
                g = jnp.dot(left, others[k].reshape(ROWS, HALF), preferred_element_type=F32)
            else:
                left = weights[:, :, pl.ds(pl.multiple_of(c * HALF, HALF), HALF)].reshape(ROWS, HALF)
                g = lax.dot_general(
                    left, others[k].reshape(ROWS, HALF), (((0,), (0,)), ((), ())), preferred_element_type=F32
                )
            g = g * multiplier
            grad[...] = g.reshape(NX * NY, 32, HALF)
            mine = grad[b].reshape(8, 4, HALF)
            which = lax.broadcasted_iota(jnp.int32, (8, 4, HALF), 0) == z
            own[side, :, k * HALF : (k + 1) * HALF] = jnp.sum(jnp.where(which, mine, 0.0), axis=0)
            u = vectors[k, c].reshape(HALF, HALF).astype(F32)
            size = size + jnp.sum(g * g, axis=1, keepdims=True)
            along = along + jnp.sum(g * u, axis=1, keepdims=True)
        length = lens[c] if side == 0 else tags[2 + c]
        inverse = 1.0 / (length * length)
        squares = squares + (size - along * along * (1.0 + EPS_UNIT * inverse)) * inverse

    swap_out[...] = jnp.broadcast_to(jnp.sum(squares, axis=0, keepdims=True), (8, 128))
    swap = remote(swap_out, swap_in, swap_sem.at[0], swap_sem.at[1], (z, x, y, 1 - c))
    swap.start()

    def own_gradient(g, unit, length):
        return (g - unit * jnp.sum(unit * g, axis=1, keepdims=True)) / length

    grad_image = own_gradient(own[0], image_unit, image_len)
    grad_text = own_gradient(own[1], text_unit, text_len)
    swap.wait_recv()
    total = swap_out[...] + swap_in[...]
    factor = lax.rsqrt(total[0:1, 0:1] * (1.0 / (2.0 * ROWS * E)) + 1e-06)
    update_image[...] = grad_image * factor
    update_text[...] = grad_text * factor
    norm[0] = jnp.sqrt(jnp.sum(total) * (1.0 / (8.0 * 128.0)))
    swap.wait_send()
    for gather in (text_gather, tag_gather, image_gather, len_gather):
        gather.drain()


def per_device(images, layer_gain, in_weight, out_weight, text_embed, pair_index, logit_scale):
    any_space = pl.BlockSpec(memory_space=pl.ANY)
    vmem = pl.BlockSpec(memory_space=pltpu.VMEM)
    smem = pl.BlockSpec(memory_space=pltpu.SMEM)
    dma = pltpu.SemaphoreType.DMA
    big = [dma((16,)), dma((16,)), dma((4,)), dma((4,)), dma((16,)), dma((16,)), dma((16,)), dma((16,))]
    small = big[:6]
    matrix = [
        pltpu.VMEM((2, 4, HALF), BF16),
        pltpu.VMEM((2 * NZ, 4, HALF), BF16),
        pltpu.VMEM((2, 2, NX * NY, 32, HALF), BF16),
    ]
    lanes = [pltpu.VMEM((1, 128), F32), pltpu.VMEM((2 * NZ, 1, 128), F32), pltpu.VMEM((NX * NY, 1, 128), F32)]
    return pl.pallas_call(
        kernel,
        out_shape=(
            jax.ShapeDtypeStruct((1,), F32),
            jax.ShapeDtypeStruct((1,), F32),
            jax.ShapeDtypeStruct((4, E), F32),
            jax.ShapeDtypeStruct((4, E), F32),
        ),
        in_specs=[any_space, vmem, any_space, any_space, vmem, smem, smem],
        out_specs=(smem, smem, vmem, vmem),
        scratch_shapes=[
            pltpu.VMEM((4, TOKENS, WIDE), BF16),
            pltpu.VMEM((4, PAD, WIDE), BF16),
            pltpu.VMEM((4, WIDE, 256), BF16),
            pltpu.VMEM((E, E), BF16),
            pltpu.VMEM((4, 8, 256), F32),
            *matrix,
            *matrix,
            *lanes,
            *lanes,
            pltpu.VMEM((ROWS, ROWS), F32),
            pltpu.VMEM((2, HALF, ROWS), BF16),
            pltpu.VMEM((ROWS, 1), F32),
            pltpu.VMEM((4, HALF, 1), F32),
            pltpu.VMEM((2, HALF, 1), F32),
            pltpu.VMEM((NX * NY, 32, HALF), F32),
            pltpu.VMEM((2, 4, E), F32),
            pltpu.VMEM((8, 128), F32),
            pltpu.VMEM((8, 128), F32),
            dma((9,)),
            dma((2,)),
            *big,
            *big,
            *small,
            *small,
        ],
        compiler_params=pltpu.CompilerParams(
            collective_id=0, has_side_effects=True, vmem_limit_bytes=63 * 1024 * 1024
        ),
        name="contrastive",
    )(images, layer_gain.reshape(1, WIDE), in_weight, out_weight, text_embed, pair_index, logit_scale)


def solution(mesh):
    torus = Mesh(mesh.devices.reshape(NZ, NX, NY, 2), AXES)
    return jax.shard_map(
        per_device,
        mesh=torus,
        in_specs=(P(AXES, None, None), P(), P(), P(), P(AXES, None), P(AXES), P()),
        out_specs=(P(), P(), P(AXES, None), P(AXES, None)),
        check_vma=False,
    )
```

```python
import jax
import jax.numpy as jnp
from jax import lax
from jax.experimental import pallas as pl
from jax.experimental.pallas import tpu as pltpu
from jax.sharding import Mesh
from jax.sharding import PartitionSpec as P

AXES = ("z", "x", "y", "c")
NZ, NX, NY = 8, 4, 4
EPS_UNIT = 1e-06
EPS_LAYER = 1e-05
F32 = jnp.float32
BF16 = jnp.bfloat16
TOKENS, WIDE, E, HALF, ROWS = 92, 4096, 1024, 512, 1024
BLOCKS = 23


def coordinates():
    return tuple(lax.axis_index(a) for a in AXES)


def remote(src, dst, send_sem, recv_sem, where):
    return pltpu.make_async_remote_copy(
        src_ref=src,
        dst_ref=dst,
        send_sem=send_sem,
        recv_sem=recv_sem,
        device_id=where,
        device_id_type=pl.DeviceIdType.MESH,
    )


Z_ORDER = (4, 3, 5, 2, 6, 1, 7, 0)
RING = (2, 1, 3)


class Gather:
    def __init__(self, place, send, line, whole, sems):
        self.z, self.x, self.y, self.c = place
        self.send, self.line, self.whole = send, line, whole
        (self.s1, self.r1, self.s2, self.r2, self.s3, self.r3, self.s4, self.r4) = sems
        self.copies = []
        self.second = {}
        self.third = {}
        self.cross = {}

    def block(self, q, p):
        c = self.c
        x = lax.rem(self.x + NX - q * (1 - c) + NX - p * c, NX)
        y = lax.rem(self.y + NY - q * c + NY - p * (1 - c), NY)
        return x * NY + y

    def start_line(self):
        j = self.c * NZ + self.z
        self.first = []
        for oz in Z_ORDER:
            for oc in range(2):
                if oz == 0 and oc == 0:
                    continue
                tz, tc = lax.rem(self.z + oz, NZ), lax.rem(self.c + oc, 2)
                o = oz * 2 + oc
                copy = remote(
                    self.send.at[tc], self.line.at[j], self.s1.at[o], self.r1.at[o], (tz, self.x, self.y, tc)
                )
                copy.start()
                self.first.append(copy)
        self.line[j] = self.send[self.c]
        self.copies += self.first

    def finish_line(self):
        for copy in self.first:
            copy.wait_recv()
        c, b = self.c, self.block(0, 0)
        for j in range(2 * NZ):
            r = (j % NZ) * 4
            self.whole[c, j // NZ, b, r : r + 4, :] = self.line[j]

    def start_second(self):
        c, b = self.c, self.block(0, 0)
        here = self.whole.at[c, :, b]
        for o in RING:
            where = (self.z, lax.rem(self.x + o * (1 - c), NX), lax.rem(self.y + o * c, NY), c)
            copy = remote(here, here, self.s2.at[o], self.r2.at[o], where)
            copy.start()
            self.second[o] = copy
            self.copies.append(copy)
        self.forward(0)

    def to_partner(self, q, p):
        here = self.whole.at[self.c, :, self.block(q, p)]
        copy = remote(here, here, self.s4.at[q * 4 + p], self.r4.at[q * 4 + p], (self.z, self.x, self.y, 1 - self.c))
        copy.start()
        self.cross[q, p] = copy
        self.copies.append(copy)

    def forward(self, q):
        c = self.c
        here = self.whole.at[c, :, self.block(q, 0)]
        for p in RING:
            where = (self.z, lax.rem(self.x + p * c, NX), lax.rem(self.y + p * (1 - c), NY), c)
            copy = remote(here, here, self.s3.at[q * 4 + p], self.r3.at[q * 4 + p], where)
            copy.start()
            self.third[q, p] = copy
            self.copies.append(copy)
        self.to_partner(q, 0)

    def finish_second(self):
        for o in (1, 3, 2):
            self.second[o].wait_recv()
            self.forward(o)

    def finish_third(self):
        for q in (0, 1, 3, 2):
            for p in (1, 3, 2):
                self.third[q, p].wait_recv()
                self.to_partner(q, p)

    def finish_cross(self):
        for q in (0, 1, 3, 2):
            for p in (0, 1, 3, 2):
                self.cross[q, p].wait_recv()

    def drain(self):
        for copy in self.copies:
            copy.wait_send()


class SmallGather:
    def __init__(self, place, send, line, whole, sems):
        self.z, self.x, self.y, self.c = place
        self.send, self.line, self.whole = send, line, whole
        (self.s1, self.r1, self.s2, self.r2, self.s3, self.r3) = sems
        self.copies = []
        self.second = {}
        self.third = {}

    block = Gather.block

    def start_line(self):
        j = self.c * NZ + self.z
        self.first = []
        for oz in Z_ORDER:
            for oc in range(2):
                if oz == 0 and oc == 0:
                    continue
                tz, tc = lax.rem(self.z + oz, NZ), lax.rem(self.c + oc, 2)
                o = oz * 2 + oc
                copy = remote(self.send, self.line.at[j], self.s1.at[o], self.r1.at[o], (tz, self.x, self.y, tc))
                copy.start()
                self.first.append(copy)
        self.line[j] = self.send[...]
        self.copies += self.first

    def finish_line(self):
        for copy in self.first:
            copy.wait_recv()
        total = self.line[0]
        for j in range(1, 2 * NZ):
            total = total + self.line[j]
        self.whole[self.block(0, 0)] = total

    def start_second(self):
        c = self.c
        here = self.whole.at[self.block(0, 0)]
        for o in RING:
            where = (self.z, lax.rem(self.x + o * (1 - c), NX), lax.rem(self.y + o * c, NY), c)
            copy = remote(here, here, self.s2.at[o], self.r2.at[o], where)
            copy.start()
            self.second[o] = copy
            self.copies.append(copy)
        self.forward(0)

    def forward(self, q):
        c = self.c
        here = self.whole.at[self.block(q, 0)]
        for p in RING:
            where = (self.z, lax.rem(self.x + p * c, NX), lax.rem(self.y + p * (1 - c), NY), c)
            copy = remote(here, here, self.s3.at[q * 4 + p], self.r3.at[q * 4 + p], where)
            copy.start()
            self.third[q, p] = copy
            self.copies.append(copy)

    def finish_second(self):
        for o in (1, 3, 2):
            self.second[o].wait_recv()
            self.forward(o)

    def finish_third(self):
        for q in (0, 1, 3, 2):
            for p in (1, 3, 2):
                self.third[q, p].wait_recv()

    drain = Gather.drain


def spread(values, first_lane):
    lanes = lax.broadcasted_iota(jnp.int32, (4, 128), 1) - lax.broadcasted_iota(jnp.int32, (4, 128), 0)
    return jnp.sum(jnp.where(lanes == first_lane, values, 0.0), axis=0, keepdims=True)


def unit_rows(matrix):
    length = jnp.sqrt(jnp.sum(matrix * matrix, axis=1, keepdims=True) + EPS_UNIT)
    return matrix / length, length


def columns_of(whole, out, kinds):
    eye = lax.broadcasted_iota(jnp.int32, (128, 128), 0) == lax.broadcasted_iota(jnp.int32, (128, 128), 1)
    for b in range(NX * NY):
        column = jnp.sum(jnp.where(eye, jnp.broadcast_to(whole[b], (128, 128)), 0.0), axis=1, keepdims=True)
        for k in range(kinds):
            out[k, b * 32 : b * 32 + 32, :] = column[k * 32 : k * 32 + 32]


def kernel(
    images, gain, in_weight, out_weight, text, pair, scale,
    loss, norm, update_image, update_text,
    pixels, normed, w, ow, pooled,
    text_send, text_line, text_all, image_send, image_line, image_all,
    tag_send, tag_line, tag_all, len_send, len_line, len_all,
    scores, weights, row_lse, tags, lens, grad, own, swap_out, swap_in,
    load_sem, swap_sem, *sems,
):
    place = coordinates()
    z, x, y, c = place
    text_gather = Gather(place, text_send, text_line, text_all, sems[0:8])
    image_gather = Gather(place, image_send, image_line, image_all, sems[8:16])
    tag_gather = SmallGather(place, tag_send, tag_line, tag_all, sems[16:22])
    len_gather = SmallGather(place, len_send, len_line, len_all, sems[22:28])

    loads = []
    for i in range(4):
        loads.append(pltpu.make_async_copy(images.at[:, i], pixels.at[:, :, pl.ds(4 * i, 4)], load_sem.at[i]))
    for n in range(4):
        part = pl.ds(n * 256, 256)
        loads.append(pltpu.make_async_copy(in_weight.at[:, part], w.at[n], load_sem.at[4 + n]))
    loads.append(pltpu.make_async_copy(out_weight, ow, load_sem.at[8]))
    for copy in loads:
        copy.start()

    barrier = pltpu.get_barrier_semaphore()
    peers = []
    for oz in range(NZ):
        for oc in range(2):
            if oz or oc:
                peers.append((lax.rem(z + oz, NZ), x, y, lax.rem(c + oc, 2)))
    for o in (1, 2, 3):
        peers.append((z, lax.rem(x + o, NX), y, c))
        peers.append((z, x, lax.rem(y + o, NY), c))
    for where in peers:
        pl.semaphore_signal(barrier, inc=1, device_id=where, device_id_type=pl.DeviceIdType.MESH)

    text_unit, text_len = unit_rows(text[...].astype(F32))
    text_vec = text_unit.astype(BF16)
    for k in range(2):
        text_send[k] = text_vec[:, k * HALF : (k + 1) * HALF]
    lane = lax.broadcasted_iota(jnp.int32, (1, 128), 1)
    first_lane = (c * NZ + z) * 4
    tag = spread(text_len, first_lane + 64)
    for i in range(4):
        t = pair[i]
        row = (((t >> 2) & 1) << 9) | (((t >> 5) & 3) << 7) | (((t >> 3) & 3) << 5) | ((t >> 7) << 2) | (t & 3)
        tag = tag + jnp.where(lane == first_lane + i, row.astype(F32), 0.0)
    tag_send[...] = tag

    pl.semaphore_wait(barrier, len(peers))
    text_gather.start_line()
    tag_gather.start_line()

    def normalise(i, carry):
        def tile(k):
            return pixels[i, k].astype(F32)

        total = jnp.zeros((16, 128), F32)
        for k in range(WIDE // 128):
            total = total + tile(k)
        average = jnp.sum(total, axis=1, keepdims=True) * (1.0 / WIDE)
        total = jnp.zeros((16, 128), F32)
        for k in range(WIDE // 128):
            centered = tile(k) - average
            total = total + centered * centered
        variance = jnp.sum(total, axis=1, keepdims=True) * (1.0 / WIDE)
        factor = lax.rsqrt(variance + EPS_LAYER)
        for k in range(WIDE // 128):
            part = slice(k * 128, (k + 1) * 128)
            normed[i, :, part] = ((tile(k) - average) * factor * gain[:, part]).astype(BF16)
        return carry

    for i in range(4):
        loads[i].wait()
    lax.fori_loop(0, BLOCKS, normalise, 0)

    text_gather.finish_line()
    tag_gather.finish_line()
    text_gather.start_second()
    tag_gather.start_second()

    pooled[...] = jnp.zeros_like(pooled)
    for n in range(4):
        loads[4 + n].wait()

    def encode(n, carry):
        flat = normed[...].reshape(BLOCKS * 16, WIDE)
        hidden = jax.nn.gelu(jnp.dot(flat, w[n], preferred_element_type=F32), approximate=True)
        pairs = jnp.sum(hidden.reshape(BLOCKS * 2, 8, 256), axis=0)
        pooled[n, 0:4, :] = (pairs[0:4] + pairs[4:8]) * (1.0 / TOKENS)
        return carry

    lax.fori_loop(0, 2, encode, 0)
    text_gather.finish_second()
    tag_gather.finish_second()
    lax.fori_loop(2, 4, encode, 0)
    loads[8].wait()
    image_emb = jnp.zeros((8, E), F32)
    for n in range(4):
        image_emb = image_emb + jnp.dot(
            pooled[n].astype(BF16), ow[n * 256 : (n + 1) * 256, :], preferred_element_type=F32
        )
    image_unit, image_len = unit_rows(image_emb[0:4])
    image_vec = image_unit.astype(BF16)
    for k in range(2):
        image_send[k] = image_vec[:, k * HALF : (k + 1) * HALF]
    len_send[...] = spread(image_len, first_lane)
    image_gather.start_line()
    len_gather.start_line()

    text_gather.finish_third()
    tag_gather.finish_third()
    columns_of(tag_all, tags, 4)
    image_gather.finish_line()
    len_gather.finish_line()
    image_gather.start_second()
    len_gather.start_second()
    text_gather.finish_cross()
    image_gather.finish_second()
    len_gather.finish_second()
    image_gather.finish_third()
    len_gather.finish_third()
    image_gather.finish_cross()
    columns_of(len_all, lens, 2)

    multiplier = scale[0]

    def score(chunk, carry):
        side, b = chunk // 2, (chunk % 2) * 8
        total = jnp.zeros((256, ROWS), F32)
        for k in range(2):
            total = total + lax.dot_general(
                image_all[k, side, pl.ds(b, 8)].reshape(256, HALF),
                text_all[k].reshape(ROWS, HALF),
                (((1,), (1,)), ((), ())),
                preferred_element_type=F32,
            )
        scores[pl.ds(pl.multiple_of(chunk * 256, 256), 256), :] = total * multiplier
        return carry

    lax.fori_loop(0, 4, score, 0)

    def over_rows(r, high):
        rows = pl.ds(pl.multiple_of(r * 32, 32), 32)
        s = scores[rows, :]
        top = jnp.max(s, axis=1, keepdims=True)
        row_lse[rows, :] = top + jnp.log(jnp.sum(jnp.exp(s - top), axis=1, keepdims=True))
        return jnp.maximum(high, jnp.max(s.reshape(4, 8, ROWS), axis=0))

    high = lax.fori_loop(0, 32, over_rows, jnp.full((8, ROWS), -jnp.inf, F32))
    high = jnp.max(high, axis=0, keepdims=True)

    def over_columns(r, total):
        rows = pl.ds(pl.multiple_of(r * 32, 32), 32)
        return total + jnp.sum(jnp.exp(scores[rows, :] - high).reshape(4, 8, ROWS), axis=0)

    total = lax.fori_loop(0, 32, over_columns, jnp.zeros((8, ROWS), F32))
    col_lse = high + jnp.log(jnp.sum(total, axis=0, keepdims=True))

    ids = lax.broadcasted_iota(jnp.int32, (32, ROWS), 1).astype(F32)

    def weigh(r, positive):
        rows = pl.ds(pl.multiple_of(r * 32, 32), 32)
        s = scores[rows, :]
        hit = ids == tags[r // 16, pl.ds(pl.multiple_of((r % 16) * 32, 32), 32), :]
        value = jnp.exp(s - row_lse[rows, :]) + jnp.exp(s - col_lse) - jnp.where(hit, 2.0, 0.0)
        weights[r // 16, pl.ds(pl.multiple_of((r % 16) * 32, 32), 32), :] = value.astype(BF16)
        return positive + jnp.sum(jnp.where(hit, s, 0.0).reshape(4, 8, ROWS), axis=0)

    positive = lax.fori_loop(0, 32, weigh, jnp.zeros((8, ROWS), F32))
    loss[0] = (jnp.sum(row_lse[...]) + jnp.sum(col_lse) - 2.0 * jnp.sum(positive)) * (0.5 / ROWS)

    squares = jnp.zeros((HALF, 1), F32)
    b = x * NY + y
    for side in range(2):
        vectors = image_all if side == 0 else text_all
        others = text_all if side == 0 else image_all
        size = jnp.zeros((HALF, 1), F32)
        along = jnp.zeros((HALF, 1), F32)
        for k in range(2):
            if side == 0:
                left = weights[c]
                g = jnp.dot(left, others[k].reshape(ROWS, HALF), preferred_element_type=F32)
            else:
                left = weights[:, :, pl.ds(pl.multiple_of(c * HALF, HALF), HALF)].reshape(ROWS, HALF)
                g = lax.dot_general(
                    left, others[k].reshape(ROWS, HALF), (((0,), (0,)), ((), ())), preferred_element_type=F32
                )
            g = g * multiplier
            grad[...] = g.reshape(NX * NY, 32, HALF)
            mine = grad[b].reshape(8, 4, HALF)
            which = lax.broadcasted_iota(jnp.int32, (8, 4, HALF), 0) == z
            own[side, :, k * HALF : (k + 1) * HALF] = jnp.sum(jnp.where(which, mine, 0.0), axis=0)
            u = vectors[k, c].reshape(HALF, HALF).astype(F32)
            size = size + jnp.sum(g * g, axis=1, keepdims=True)
            along = along + jnp.sum(g * u, axis=1, keepdims=True)
        length = lens[c] if side == 0 else tags[2 + c]
        inverse = 1.0 / (length * length)
        squares = squares + (size - along * along * (1.0 + EPS_UNIT * inverse)) * inverse

    swap_out[...] = jnp.broadcast_to(jnp.sum(squares, axis=0, keepdims=True), (8, 128))
    swap = remote(swap_out, swap_in, swap_sem.at[0], swap_sem.at[1], (z, x, y, 1 - c))
    swap.start()

    def own_gradient(g, unit, length):
        return (g - unit * jnp.sum(unit * g, axis=1, keepdims=True)) / length

    grad_image = own_gradient(own[0], image_unit, image_len)
    grad_text = own_gradient(own[1], text_unit, text_len)
    swap.wait_recv()
    total = swap_out[...] + swap_in[...]
    factor = lax.rsqrt(total[0:1, 0:1] * (1.0 / (2.0 * ROWS * E)) + 1e-06)
    update_image[...] = grad_image * factor
    update_text[...] = grad_text * factor
    norm[0] = jnp.sqrt(jnp.sum(total) * (1.0 / (8.0 * 128.0)))
    swap.wait_send()
    for gather in (text_gather, tag_gather, image_gather, len_gather):
        gather.drain()


def per_device(images, layer_gain, in_weight, out_weight, text_embed, pair_index, logit_scale):
    any_space = pl.BlockSpec(memory_space=pl.ANY)
    vmem = pl.BlockSpec(memory_space=pltpu.VMEM)
    smem = pl.BlockSpec(memory_space=pltpu.SMEM)
    dma = pltpu.SemaphoreType.DMA
    big = [dma((16,)), dma((16,)), dma((4,)), dma((4,)), dma((16,)), dma((16,)), dma((16,)), dma((16,))]
    small = big[:6]
    matrix = [
        pltpu.VMEM((2, 4, HALF), BF16),
        pltpu.VMEM((2 * NZ, 4, HALF), BF16),
        pltpu.VMEM((2, 2, NX * NY, 32, HALF), BF16),
    ]
    lanes = [pltpu.VMEM((1, 128), F32), pltpu.VMEM((2 * NZ, 1, 128), F32), pltpu.VMEM((NX * NY, 1, 128), F32)]
    return pl.pallas_call(
        kernel,
        out_shape=(
            jax.ShapeDtypeStruct((1,), F32),
            jax.ShapeDtypeStruct((1,), F32),
            jax.ShapeDtypeStruct((4, E), F32),
            jax.ShapeDtypeStruct((4, E), F32),
        ),
        in_specs=[any_space, vmem, any_space, any_space, vmem, smem, smem],
        out_specs=(smem, smem, vmem, vmem),
        scratch_shapes=[
            pltpu.VMEM((BLOCKS, WIDE // 128, 16, 128), BF16),
            pltpu.VMEM((BLOCKS, 16, WIDE), BF16),
            pltpu.VMEM((4, WIDE, 256), BF16),
            pltpu.VMEM((E, E), BF16),
            pltpu.VMEM((4, 8, 256), F32),
            *matrix,
            *matrix,
            *lanes,
            *lanes,
            pltpu.VMEM((ROWS, ROWS), F32),
            pltpu.VMEM((2, HALF, ROWS), BF16),
            pltpu.VMEM((ROWS, 1), F32),
            pltpu.VMEM((4, HALF, 1), F32),
            pltpu.VMEM((2, HALF, 1), F32),
            pltpu.VMEM((NX * NY, 32, HALF), F32),
            pltpu.VMEM((2, 4, E), F32),
            pltpu.VMEM((8, 128), F32),
            pltpu.VMEM((8, 128), F32),
            dma((9,)),
            dma((2,)),
            *big,
            *big,
            *small,
            *small,
        ],
        compiler_params=pltpu.CompilerParams(
            collective_id=0, has_side_effects=True, vmem_limit_bytes=63 * 1024 * 1024
        ),
        name="contrastive",
    )(images.reshape(4, BLOCKS, 4, WIDE // 128, 128).transpose(1, 2, 3, 0, 4), layer_gain.reshape(1, WIDE), in_weight, out_weight, text_embed, pair_index, logit_scale)


def solution(mesh):
    torus = Mesh(mesh.devices.reshape(NZ, NX, NY, 2), AXES)
    return jax.shard_map(
        per_device,
        mesh=torus,
        in_specs=(P(AXES, None, None), P(), P(), P(), P(AXES, None), P(AXES), P()),
        out_specs=(P(), P(), P(AXES, None), P(AXES, None)),
        check_vma=False,
    )
```

```python
import jax
import jax.numpy as jnp
from jax import lax
from jax.experimental import pallas as pl
from jax.experimental.pallas import tpu as pltpu
from jax.sharding import Mesh
from jax.sharding import PartitionSpec as P

AXES = ("z", "x", "y", "c")
NZ, NX, NY = 8, 4, 4
EPS_UNIT = 1e-06
EPS_LAYER = 1e-05
F32 = jnp.float32
BF16 = jnp.bfloat16
TOKENS, WIDE, E, HALF, ROWS = 92, 4096, 1024, 512, 1024
BLOCKS = 23
GROUPS = ((0, 8), (8, 8), (16, 7))
LOG2E = 1.4426950408889634
LN2 = 0.6931471805599453


def coordinates():
    return tuple(lax.axis_index(a) for a in AXES)


def remote(src, dst, send_sem, recv_sem, where):
    return pltpu.make_async_remote_copy(
        src_ref=src,
        dst_ref=dst,
        send_sem=send_sem,
        recv_sem=recv_sem,
        device_id=where,
        device_id_type=pl.DeviceIdType.MESH,
    )


Z_ORDER = (4, 3, 5, 2, 6, 1, 7, 0)
RING = (2, 1, 3)


class Gather:
    def __init__(self, place, send, line, whole, sems):
        self.z, self.x, self.y, self.c = place
        self.send, self.line, self.whole = send, line, whole
        (self.s1, self.r1, self.s2, self.r2, self.s3, self.r3, self.s4, self.r4) = sems
        self.copies = []
        self.second = {}
        self.third = {}
        self.cross = {}

    def block(self, q, p):
        c = self.c
        x = lax.rem(self.x + NX - q * (1 - c) + NX - p * c, NX)
        y = lax.rem(self.y + NY - q * c + NY - p * (1 - c), NY)
        return x * NY + y

    def start_line(self):
        j = self.c * NZ + self.z
        self.first = []
        for oz in Z_ORDER:
            for oc in range(2):
                if oz == 0 and oc == 0:
                    continue
                tz, tc = lax.rem(self.z + oz, NZ), lax.rem(self.c + oc, 2)
                o = oz * 2 + oc
                copy = remote(
                    self.send.at[tc], self.line.at[j], self.s1.at[o], self.r1.at[o], (tz, self.x, self.y, tc)
                )
                copy.start()
                self.first.append(copy)
        self.line[j] = self.send[self.c]
        self.copies += self.first

    def finish_line(self):
        for copy in self.first:
            copy.wait_recv()
        c, b = self.c, self.block(0, 0)
        for j in range(2 * NZ):
            r = (j % NZ) * 4
            self.whole[c, j // NZ, b, r : r + 4, :] = self.line[j]

    def start_second(self):
        c, b = self.c, self.block(0, 0)
        here = self.whole.at[c, :, b]
        for o in RING:
            where = (self.z, lax.rem(self.x + o * (1 - c), NX), lax.rem(self.y + o * c, NY), c)
            copy = remote(here, here, self.s2.at[o], self.r2.at[o], where)
            copy.start()
            self.second[o] = copy
            self.copies.append(copy)
        self.forward(0)

    def to_partner(self, q, p):
        here = self.whole.at[self.c, :, self.block(q, p)]
        copy = remote(here, here, self.s4.at[q * 4 + p], self.r4.at[q * 4 + p], (self.z, self.x, self.y, 1 - self.c))
        copy.start()
        self.cross[q, p] = copy
        self.copies.append(copy)

    def forward(self, q):
        c = self.c
        here = self.whole.at[c, :, self.block(q, 0)]
        for p in RING:
            where = (self.z, lax.rem(self.x + p * c, NX), lax.rem(self.y + p * (1 - c), NY), c)
            copy = remote(here, here, self.s3.at[q * 4 + p], self.r3.at[q * 4 + p], where)
            copy.start()
            self.third[q, p] = copy
            self.copies.append(copy)
        self.to_partner(q, 0)

    def finish_second(self):
        for o in (1, 3, 2):
            self.second[o].wait_recv()
            self.forward(o)

    def finish_third(self):
        for q in (0, 1, 3, 2):
            for p in (1, 3, 2):
                self.third[q, p].wait_recv()
                self.to_partner(q, p)

    def finish_cross(self):
        for q in (0, 1, 3, 2):
            for p in (0, 1, 3, 2):
                self.cross[q, p].wait_recv()

    def drain(self):
        for copy in self.copies:
            copy.wait_send()


class SmallGather:
    def __init__(self, place, send, line, whole, sems):
        self.z, self.x, self.y, self.c = place
        self.send, self.line, self.whole = send, line, whole
        (self.s1, self.r1, self.s2, self.r2, self.s3, self.r3) = sems
        self.copies = []
        self.second = {}
        self.third = {}

    block = Gather.block

    def start_line(self):
        j = self.c * NZ + self.z
        self.first = []
        for oz in Z_ORDER:
            for oc in range(2):
                if oz == 0 and oc == 0:
                    continue
                tz, tc = lax.rem(self.z + oz, NZ), lax.rem(self.c + oc, 2)
                o = oz * 2 + oc
                copy = remote(self.send, self.line.at[j], self.s1.at[o], self.r1.at[o], (tz, self.x, self.y, tc))
                copy.start()
                self.first.append(copy)
        self.line[j] = self.send[...]
        self.copies += self.first

    def finish_line(self):
        for copy in self.first:
            copy.wait_recv()
        total = self.line[0]
        for j in range(1, 2 * NZ):
            total = total + self.line[j]
        self.whole[self.block(0, 0)] = total

    def start_second(self):
        c = self.c
        here = self.whole.at[self.block(0, 0)]
        for o in RING:
            where = (self.z, lax.rem(self.x + o * (1 - c), NX), lax.rem(self.y + o * c, NY), c)
            copy = remote(here, here, self.s2.at[o], self.r2.at[o], where)
            copy.start()
            self.second[o] = copy
            self.copies.append(copy)
        self.forward(0)

    def forward(self, q):
        c = self.c
        here = self.whole.at[self.block(q, 0)]
        for p in RING:
            where = (self.z, lax.rem(self.x + p * c, NX), lax.rem(self.y + p * (1 - c), NY), c)
            copy = remote(here, here, self.s3.at[q * 4 + p], self.r3.at[q * 4 + p], where)
            copy.start()
            self.third[q, p] = copy
            self.copies.append(copy)

    def finish_second(self):
        for o in (1, 3, 2):
            self.second[o].wait_recv()
            self.forward(o)

    def finish_third(self):
        for q in (0, 1, 3, 2):
            for p in (1, 3, 2):
                self.third[q, p].wait_recv()

    drain = Gather.drain


def spread(values, first_lane):
    lanes = lax.broadcasted_iota(jnp.int32, (4, 128), 1) - lax.broadcasted_iota(jnp.int32, (4, 128), 0)
    return jnp.sum(jnp.where(lanes == first_lane, values, 0.0), axis=0, keepdims=True)


def unit_rows(matrix):
    length = jnp.sqrt(jnp.sum(matrix * matrix, axis=1, keepdims=True) + EPS_UNIT)
    return matrix / length, length


def columns_of(whole, out, kinds):
    eye = lax.broadcasted_iota(jnp.int32, (128, 128), 0) == lax.broadcasted_iota(jnp.int32, (128, 128), 1)
    for b in range(NX * NY):
        column = jnp.sum(jnp.where(eye, jnp.broadcast_to(whole[b], (128, 128)), 0.0), axis=1, keepdims=True)
        for k in range(kinds):
            out[k, b * 32 : b * 32 + 32, :] = jnp.broadcast_to(column[k * 32 : k * 32 + 32], (32, 128))


def kernel(
    images, gain_in, in_weight, out_weight, text_in, pair_in, scale_in,
    loss, norm, update_image, update_text,
    pixels, normed, w, ow, pooled, gain, text, pair, scale,
    text_send, text_line, text_all, image_send, image_line, image_all,
    tag_send, tag_line, tag_all, len_send, len_line, len_all,
    text_turned, turned_lse, scores, weights, row_high, row_part, row_lse, tags, lens, grad, own, swap_out, swap_in,
    load_sem, swap_sem, *sems,
):
    place = coordinates()
    z, x, y, c = place
    text_gather = Gather(place, text_send, text_line, text_all, sems[0:8])
    image_gather = Gather(place, image_send, image_line, image_all, sems[8:16])
    tag_gather = SmallGather(place, tag_send, tag_line, tag_all, sems[16:22])
    len_gather = SmallGather(place, len_send, len_line, len_all, sems[22:28])

    small = []
    for i, (source, target) in enumerate(((text_in, text), (pair_in, pair), (gain_in, gain), (scale_in, scale))):
        small.append(pltpu.make_async_copy(source, target, load_sem.at[i]))
    pieces = []
    for n, (start, size) in enumerate(GROUPS):
        for i in range(4):
            block = pl.ds(start, size)
            pieces.append(
                pltpu.make_async_copy(
                    images.at[block, i], pixels.at[block, :, pl.ds(4 * i, 4)], load_sem.at[4 + 4 * n + i]
                )
            )
    loads = []
    for n in range(4):
        part = pl.ds(n * 256, 256)
        loads.append(pltpu.make_async_copy(in_weight.at[:, part], w.at[n], load_sem.at[16 + n]))
    loads.append(pltpu.make_async_copy(out_weight, ow, load_sem.at[20]))
    for copy in small + pieces + loads:
        copy.start()

    barrier = pltpu.get_barrier_semaphore()
    peers = []
    for oz in range(NZ):
        for oc in range(2):
            if oz or oc:
                peers.append((lax.rem(z + oz, NZ), x, y, lax.rem(c + oc, 2)))
    for o in (1, 2, 3):
        peers.append((z, lax.rem(x + o, NX), y, c))
        peers.append((z, x, lax.rem(y + o, NY), c))
    for where in peers:
        pl.semaphore_signal(barrier, inc=1, device_id=where, device_id_type=pl.DeviceIdType.MESH)

    small[0].wait()
    small[1].wait()
    text_unit, text_len = unit_rows(text[...].astype(F32))
    text_vec = text_unit.astype(BF16)
    for k in range(2):
        text_send[k] = text_vec[:, k * HALF : (k + 1) * HALF]
    lane = lax.broadcasted_iota(jnp.int32, (1, 128), 1)
    first_lane = (c * NZ + z) * 4
    tag = spread(text_len, first_lane + 64)
    for i in range(4):
        t = pair[i]
        row = (((t >> 2) & 1) << 9) | (((t >> 5) & 3) << 7) | (((t >> 3) & 3) << 5) | ((t >> 7) << 2) | (t & 3)
        tag = tag + jnp.where(lane == first_lane + i, row.astype(F32), 0.0)
    tag_send[...] = tag

    def normalise(start, size):
        def tile(k):
            return pixels[start : start + size, k].astype(F32)

        shift = jnp.sum(tile(0), axis=2, keepdims=True) * (1.0 / 128)
        total = jnp.zeros((size, 16, 128), F32)
        square = jnp.zeros((size, 16, 128), F32)
        for k in range(WIDE // 128):
            moved = tile(k) - shift
            total = total + moved
            square = square + moved * moved
        moved = jnp.sum(total, axis=2, keepdims=True) * (1.0 / WIDE)
        variance = jnp.sum(square, axis=2, keepdims=True) * (1.0 / WIDE) - moved * moved
        factor = lax.rsqrt(jnp.maximum(variance, 0.0) + EPS_LAYER)
        average = shift + moved
        for k in range(WIDE // 128):
            part = slice(k * 128, (k + 1) * 128)
            normed[start : start + size, :, part] = ((tile(k) - average) * factor * gain[:, part]).astype(BF16)

    small[2].wait()
    small[3].wait()
    for n, (start, size) in enumerate(GROUPS):
        for copy in pieces[4 * n : 4 * n + 4]:
            copy.wait()
        if n == 1:
            pl.semaphore_wait(barrier, len(peers))
            text_gather.start_line()
            tag_gather.start_line()
        normalise(start, size)

    pooled[...] = jnp.zeros_like(pooled)
    for n in range(4):
        loads[n].wait()

    def encode(n, carry):
        flat = normed[...].reshape(BLOCKS * 16, WIDE)
        hidden = jax.nn.gelu(jnp.dot(flat, w[n], preferred_element_type=F32), approximate=True)
        pairs = jnp.sum(hidden.reshape(BLOCKS * 2, 8, 256), axis=0)
        pooled[n, 0:4, :] = (pairs[0:4] + pairs[4:8]) * (1.0 / TOKENS)
        return carry

    lax.fori_loop(0, 3, encode, 0)
    text_gather.finish_line()
    tag_gather.finish_line()
    text_gather.start_second()
    tag_gather.start_second()
    lax.fori_loop(3, 4, encode, 0)
    loads[4].wait()
    image_emb = jnp.zeros((8, E), F32)
    for n in range(4):
        image_emb = image_emb + jnp.dot(
            pooled[n].astype(BF16), ow[n * 256 : (n + 1) * 256, :], preferred_element_type=F32
        )
    image_unit, image_len = unit_rows(image_emb[0:4])
    image_vec = image_unit.astype(BF16)
    for k in range(2):
        image_send[k] = image_vec[:, k * HALF : (k + 1) * HALF]
    len_send[...] = spread(image_len, first_lane)
    image_gather.start_line()
    len_gather.start_line()

    text_gather.finish_second()
    tag_gather.finish_second()
    image_gather.finish_line()
    len_gather.finish_line()
    image_gather.start_second()
    len_gather.start_second()
    text_gather.finish_third()
    tag_gather.finish_third()
    image_gather.finish_second()
    len_gather.finish_second()
    text_gather.finish_cross()
    columns_of(tag_all, tags, 4)
    for k in range(2):
        for n in range(8):
            rows = text_all[k].reshape(ROWS, HALF)[n * 128 : (n + 1) * 128]
            text_turned[k, :, n * 128 : (n + 1) * 128] = rows.T
    image_gather.finish_third()
    len_gather.finish_third()
    columns_of(len_all, lens, 2)
    image_gather.finish_cross()

    multiplier = scale[0]
    high = jnp.full((8, ROWS), -jnp.inf, F32)
    for n in range(4):
        side, b = n // 2, (n % 2) * 8
        total = jnp.zeros((256, ROWS), F32)
        for k in range(2):
            vectors = image_all[k, side, b : b + 8].reshape(256, HALF)
            total = total + jnp.dot(vectors, text_turned[k], preferred_element_type=F32)
        total = total * (multiplier * LOG2E)
        rows = slice(n * 256, (n + 1) * 256)
        scores[rows, :] = total
        top = total[:, 0:128]
        for t in range(1, 8):
            top = jnp.maximum(top, total[:, t * 128 : (t + 1) * 128])
        row_high[rows, :] = jnp.broadcast_to(jnp.max(top, axis=1, keepdims=True), (256, 128))
        high = jnp.maximum(high, jnp.max(total.reshape(32, 8, ROWS), axis=0))
    high = jnp.max(high, axis=0, keepdims=True)

    def sums(r, total):
        rows = pl.ds(pl.multiple_of(r * 32, 32), 32)
        top = row_high[rows, :]
        part = jnp.zeros((32, 128), F32)
        down = []
        for t in range(8):
            lanes = slice(t * 128, (t + 1) * 128)
            s = scores[rows, lanes]
            part = part + jnp.exp2(s - top)
            down.append(jnp.sum(jnp.exp2(s - high[:, lanes]).reshape(4, 8, 128), axis=0))
        row_part[rows, :] = part
        return total + jnp.concatenate(down, axis=1)

    total = lax.fori_loop(0, 32, sums, jnp.zeros((8, ROWS), F32))
    col_lse = high + jnp.log2(jnp.sum(total, axis=0, keepdims=True))
    row_sum = jnp.sum(row_part[...], axis=1, keepdims=True)
    row_lse[...] = row_high[...] + jnp.log2(jnp.broadcast_to(row_sum, (ROWS, 128)))

    lane = lax.broadcasted_iota(jnp.int32, (1, 128), 1).astype(F32)

    def weigh_own(r, positive):
        at = pl.multiple_of(r * 32, 32)
        rows = pl.ds(pl.multiple_of(c * HALF + at, 32), 32)
        tag, lse = tags[c, pl.ds(at, 32), :], row_lse[rows, :]
        for t in range(8):
            lanes = slice(t * 128, (t + 1) * 128)
            s = scores[rows, lanes]
            hit = tag == lane + (t * 128.0)
            value = jnp.exp2(s - lse) + jnp.exp2(s - col_lse[:, lanes]) - jnp.where(hit, 2.0, 0.0)
            weights[c, pl.ds(at, 32), lanes] = value.astype(BF16)
            positive = positive + jnp.where(hit, s, 0.0)
        return positive

    positive = lax.fori_loop(0, 16, weigh_own, jnp.zeros((32, 128), F32))
    turned_lse[...] = col_lse
    d = 1 - c

    def weigh_other(r, carry):
        at = pl.multiple_of(r * 32, 32)
        rows = pl.ds(pl.multiple_of(d * HALF + at, 32), 32)
        tag, lse = tags[d, pl.ds(at, 32), :] - (c * HALF).astype(F32), row_lse[rows, :]
        for t in range(4):
            lanes = pl.ds(pl.multiple_of(c * HALF + t * 128, 128), 128)
            s = scores[rows, lanes]
            hit = tag == lane + (t * 128.0)
            value = jnp.exp2(s - lse) + jnp.exp2(s - turned_lse[:, lanes]) - jnp.where(hit, 2.0, 0.0)
            weights[d, pl.ds(at, 32), lanes] = value.astype(BF16)
        return carry

    lax.fori_loop(0, 16, weigh_other, 0)

    squares = jnp.zeros((HALF, 1), F32)
    b = x * NY + y
    for side in range(2):
        vectors = image_all if side == 0 else text_all
        others = text_all if side == 0 else image_all
        size = jnp.zeros((HALF, 1), F32)
        along = jnp.zeros((HALF, 1), F32)
        for k in range(2):
            if side == 0:
                left = weights[c]
                g = jnp.dot(left, others[k].reshape(ROWS, HALF), preferred_element_type=F32)
            else:
                left = weights[:, :, pl.ds(pl.multiple_of(c * HALF, HALF), HALF)].reshape(ROWS, HALF)
                g = lax.dot_general(
                    left, others[k].reshape(ROWS, HALF), (((0,), (0,)), ((), ())), preferred_element_type=F32
                )
            g = g * multiplier
            grad[...] = g.reshape(NX * NY, 32, HALF)
            mine = grad[b].reshape(8, 4, HALF)
            which = lax.broadcasted_iota(jnp.int32, (8, 4, HALF), 0) == z
            own[side, :, k * HALF : (k + 1) * HALF] = jnp.sum(jnp.where(which, mine, 0.0), axis=0)
            u = vectors[k, c].reshape(HALF, HALF).astype(F32)
            size = size + jnp.sum(g * g, axis=1, keepdims=True)
            along = along + jnp.sum(g * u, axis=1, keepdims=True)
        length = lens[c, :, 0:1] if side == 0 else tags[2 + c, :, 0:1]
        inverse = 1.0 / (length * length)
        squares = squares + (size - along * along * (1.0 + EPS_UNIT * inverse)) * inverse

    swap_out[0] = jnp.broadcast_to(jnp.sum(squares, axis=0, keepdims=True), (8, 128))
    swap_out[1] = jnp.broadcast_to(jnp.sum(jnp.sum(positive, axis=0, keepdims=True), axis=1, keepdims=True), (8, 128))
    swap = remote(swap_out, swap_in, swap_sem.at[0], swap_sem.at[1], (z, x, y, 1 - c))
    swap.start()

    def own_gradient(g, unit, length):
        return (g - unit * jnp.sum(unit * g, axis=1, keepdims=True)) / length

    grad_image = own_gradient(own[0], image_unit, image_len)
    grad_text = own_gradient(own[1], text_unit, text_len)
    spread_lse = jnp.sum(row_lse[...]) * (1.0 / 128) + jnp.sum(col_lse)
    swap.wait_recv()
    total = (swap_out[0] + swap_in[0])[0:1, 0:1]
    factor = lax.rsqrt(total * (1.0 / (2.0 * ROWS * E)) + 1e-06)
    update_image[...] = grad_image * factor
    update_text[...] = grad_text * factor
    norm[0] = jnp.sum(jnp.sqrt(total))
    loss[0] = (spread_lse - 2.0 * jnp.sum((swap_out[1] + swap_in[1])[0:1, 0:1])) * (LN2 * 0.5 / ROWS)
    swap.wait_send()
    for gather in (text_gather, tag_gather, image_gather, len_gather):
        gather.drain()


def per_device(images, layer_gain, in_weight, out_weight, text_embed, pair_index, logit_scale):
    any_space = pl.BlockSpec(memory_space=pl.ANY)
    vmem = pl.BlockSpec(memory_space=pltpu.VMEM)
    smem = pl.BlockSpec(memory_space=pltpu.SMEM)
    dma = pltpu.SemaphoreType.DMA
    big = [dma((16,)), dma((16,)), dma((4,)), dma((4,)), dma((16,)), dma((16,)), dma((16,)), dma((16,))]
    small = big[:6]
    matrix = [
        pltpu.VMEM((2, 4, HALF), BF16),
        pltpu.VMEM((2 * NZ, 4, HALF), BF16),
        pltpu.VMEM((2, 2, NX * NY, 32, HALF), BF16),
    ]
    lanes = [pltpu.VMEM((1, 128), F32), pltpu.VMEM((2 * NZ, 1, 128), F32), pltpu.VMEM((NX * NY, 1, 128), F32)]
    return pl.pallas_call(
        kernel,
        out_shape=(
            jax.ShapeDtypeStruct((1,), F32),
            jax.ShapeDtypeStruct((1,), F32),
            jax.ShapeDtypeStruct((4, E), F32),
            jax.ShapeDtypeStruct((4, E), F32),
        ),
        in_specs=[any_space] * 7,
        out_specs=(smem, smem, vmem, vmem),
        scratch_shapes=[
            pltpu.VMEM((BLOCKS, WIDE // 128, 16, 128), BF16),
            pltpu.VMEM((BLOCKS, 16, WIDE), BF16),
            pltpu.VMEM((4, WIDE, 256), BF16),
            pltpu.VMEM((E, E), BF16),
            pltpu.VMEM((4, 8, 256), F32),
            pltpu.VMEM((1, WIDE), F32),
            pltpu.VMEM((4, E), BF16),
            pltpu.SMEM((4,), jnp.int32),
            pltpu.SMEM((1,), F32),
            *matrix,
            *matrix,
            *lanes,
            *lanes,
            pltpu.VMEM((2, HALF, ROWS), BF16),
            pltpu.VMEM((1, ROWS), F32),
            pltpu.VMEM((ROWS, ROWS), F32),
            pltpu.VMEM((2, HALF, ROWS), BF16),
            pltpu.VMEM((ROWS, 128), F32),
            pltpu.VMEM((ROWS, 128), F32),
            pltpu.VMEM((ROWS, 128), F32),
            pltpu.VMEM((4, HALF, 128), F32),
            pltpu.VMEM((2, HALF, 128), F32),
            pltpu.VMEM((NX * NY, 32, HALF), F32),
            pltpu.VMEM((2, 4, E), F32),
            pltpu.VMEM((2, 8, 128), F32),
            pltpu.VMEM((2, 8, 128), F32),
            dma((21,)),
            dma((2,)),
            *big,
            *big,
            *small,
            *small,
        ],
        compiler_params=pltpu.CompilerParams(
            collective_id=0, has_side_effects=True, vmem_limit_bytes=63 * 1024 * 1024
        ),
        name="contrastive",
    )(images.reshape(4, BLOCKS, 4, WIDE // 128, 128).transpose(1, 2, 3, 0, 4), layer_gain.reshape(1, WIDE), in_weight, out_weight, text_embed, pair_index, logit_scale)


def solution(mesh):
    torus = Mesh(mesh.devices.reshape(NZ, NX, NY, 2), AXES)
    return jax.shard_map(
        per_device,
        mesh=torus,
        in_specs=(P(AXES, None, None), P(), P(), P(), P(AXES, None), P(AXES), P()),
        out_specs=(P(), P(), P(AXES, None), P(AXES, None)),
        check_vma=False,
    )
```
